32 devices in a mesh: clip: 16 (over z, x, core), tm: 2 (over y).
Axes of the slice: x: 2, y: 2, z: 4, core: 2. Of those that a mesh axis runs over, the one named last changes fastest.
Arguments:
- block_input: bfloat16 [16, 4, 32, 4096], P('clip', 'tm'), may hold values from -6 to 6
- input_cache: bfloat16 [16, 2, 32, 4096], P('clip'), may hold values from -6 to 6
- middle_cache: bfloat16 [16, 2, 32, 4096], P('clip'), may hold values from -6 to 6
- first_weight: bfloat16 [3, 3, 3, 64, 64], replicated, may hold values from -0.15625 to 0.15625
- first_bias: float32 [64], replicated, may hold values from -3 to 3
- second_weight: bfloat16 [3, 3, 3, 64, 64], replicated, may hold values from -0.15625 to 0.15625
- cotangent: bfloat16 [16, 4, 32, 4096], P('clip', 'tm'), may hold values from -6 to 6
Outputs:
- input_grad: bfloat16 [16, 4, 32, 4096], P('clip', 'tm')
- input_cache_grad: bfloat16 [16, 2, 32, 4096], P('clip', None, 'tm')
- middle_cache_grad: bfloat16 [16, 2, 32, 4096], P('clip', None, 'tm')
- first_weight_grad: float32 [3, 3, 3, 64, 64], replicated
- second_weight_grad: float32 [3, 3, 3, 64, 64], replicated
The draws below stay inside these ranges and needn't reach their ends.
All inputs are finite; a program needn't handle non-finite values.
Results may differ from the reference program's by a relative error of at most 0.009.
Values may be sent and summed in bfloat16 or wider, within the bound.
No kernel may reach another device: no remote copies, remote signals or barrier semaphores. Data moves between devices by JAX's collectives and lax.ppermute only.
A program may use at most 128 MiB of HBM per device.

```python
import jax
import jax.numpy as jnp
from jax import lax

C = 64
H = 32
W = 64
CLIPS = 16
FRAMES = 4


def steps_of(key, extent, pieces, smallest, high):
    factor_of, own = 1.0, jax.random.fold_in(key, 6)
    for position, blocks in pieces:
        heights = jnp.exp(jax.random.uniform(jax.random.fold_in(own, position), (blocks,), jnp.float32, smallest / len(pieces), high / len(pieces)))
        factor_of = factor_of * jnp.repeat(heights, extent[position] // blocks).reshape([-1 if axis == position else 1 for axis in range(len(extent))])
    return factor_of


def normal_values(key, shape, scale, limit, shards=(), kind=jnp.bfloat16):
    result = jax.random.normal(key, shape, jnp.float32) * scale
    if len(shards) > 0:
        result = steps_of(key, shape, shards, -0.22, 0.18) * result
    return jnp.clip(result, min=-limit, max=limit).astype(kind)


def setup_inputs(seed: int = 0) -> dict:
    key_of = jax.random.split(jax.random.key(seed), 8)
    return {
        "block_input": normal_values(key_of[0], (CLIPS, FRAMES, H, W * C), 1.0, 6.0, ((0, 16), (1, 2))),
        "input_cache": normal_values(key_of[1], (CLIPS, 2, H, W * C), 1.0, 6.0, ((0, 16),)),
        "middle_cache": normal_values(key_of[2], (CLIPS, 2, H, W * C), 1.0, 6.0, ((0, 16),)),
        "first_weight": normal_values(key_of[3], (3, 3, 3, C, C), (27 * C) ** -0.5, 0.15625),
        "first_bias": normal_values(key_of[4], (C,), 0.5, 3.0, (), jnp.float32),
        "second_weight": normal_values(key_of[5], (3, 3, 3, C, C), (27 * C) ** -0.5, 0.15625),
        "cotangent": normal_values(key_of[6], (CLIPS, FRAMES, H, W * C), 1.0, 6.0, ((0, 16), (1, 2))),
    }


def conv(source, weight):
    return lax.conv_general_dilated(source.astype(jnp.float32), weight.astype(jnp.float32), (1, 1, 1), ((0, 0), (1, 1), (1, 1)), dimension_numbers=('NDHWC', 'DHWIO', 'NDHWC'), precision=lax.Precision.HIGHEST)

def silu_slope(value):
    logistic = jax.nn.sigmoid(value)
    return logistic * (1.0 + value * (1.0 - logistic))

def reference(block_input, input_cache, middle_cache, first_weight, first_bias, second_weight, cotangent):

    def one_clip(items):
        block, cache_first, cache_second, upstream = items
        shaped = block.reshape(1, FRAMES, H, W, C)
        extended = jnp.concatenate([cache_first.reshape(1, 2, H, W, C), shaped], axis=1)
        activated = jax.nn.silu(extended.astype(jnp.float32)).astype(jnp.bfloat16)
        pre = conv(activated, first_weight) + first_bias
        middle = jax.nn.silu(pre).astype(jnp.bfloat16)
        middle_ext = jnp.concatenate([cache_second.reshape(1, 2, H, W, C), middle], axis=1)
        upstream_f = upstream.reshape(1, FRAMES, H, W, C).astype(jnp.float32)
        unused_out, pull_second = jax.vjp(conv, middle_ext.astype(jnp.float32), second_weight.astype(jnp.float32))
        middle_ext_grad, second_sum = pull_second(upstream_f)
        pre_grad = (middle_ext_grad[:, 2:] * silu_slope(pre)).astype(jnp.bfloat16)
        unused_pre, pull_first = jax.vjp(conv, activated.astype(jnp.float32), first_weight.astype(jnp.float32))
        activated_grad, first_sum = pull_first(pre_grad.astype(jnp.float32))
        extended_grad = activated_grad * silu_slope(extended.astype(jnp.float32))
        input_grad = (upstream_f + extended_grad[:, 2:]).astype(jnp.bfloat16).reshape(FRAMES, H, W * C)
        input_cache_grad = extended_grad[:, :2].astype(jnp.bfloat16).reshape(2, H, W * C)
        middle_cache_grad = middle_ext_grad[:, :2].astype(jnp.bfloat16).reshape(2, H, W * C)
        return (input_grad, input_cache_grad, middle_cache_grad, first_sum, second_sum)
    grads, cache_a, cache_b, first_all, second_all = lax.map(one_clip, (block_input, input_cache, middle_cache, cotangent))
    factor = 1.0 / jnp.sqrt(jnp.float32(CLIPS * FRAMES * H * W))
    first_weight_grad = lax.optimization_barrier(jnp.sum(first_all, axis=0)) * factor
    second_weight_grad = lax.optimization_barrier(jnp.sum(second_all, axis=0)) * factor
    return (grads, cache_a, cache_b, first_weight_grad, second_weight_grad)
```

```python
import functools
import math

import jax
import jax.numpy as jnp
from jax import lax
from jax.experimental import pallas as pl
from jax.experimental.pallas import tpu as pltpu
from jax.sharding import PartitionSpec as P

F32 = jnp.float32
BF16 = jnp.bfloat16
OUT = 256
WIN = 384
VMEM = pl.BlockSpec(memory_space=pltpu.VMEM)
SMEM = pl.BlockSpec(memory_space=pltpu.SMEM)
PARAMS = pltpu.CompilerParams(vmem_limit_bytes=60 * 1024 * 1024)


def logistic(value):
    return 1.0 / (1.0 + jnp.exp(-value))


def slope_of(value):
    s = logistic(value)
    return s * (1.0 + value * (1.0 - s))


def row_shifts(value):
    rows = value.shape[0]
    row = lax.broadcasted_iota(jnp.int32, value.shape, 0)
    down = jnp.where(row == 0, 0.0, pltpu.roll(value, 1, axis=0))
    up = jnp.where(row == rows - 1, 0.0, pltpu.roll(value, rows - 1, axis=0))
    return down, value, up


def column_shift(value, chans):
    pad = jnp.zeros((value.shape[0], 2 * chans), value.dtype)
    return pltpu.roll(jnp.concatenate([value, pad], axis=1), chans, axis=1)


def put_shifted(ref, frame, value, chans):
    for k, part in enumerate(row_shifts(column_shift(value, chans))):
        ref[frame, k] = part.astype(BF16)


def banded(weight):
    chans = weight.shape[3]
    left = jnp.pad(weight, ((0, 0), (0, 0), (0, 1), (0, 0), (0, 0)))
    right = jnp.pad(weight, ((0, 0), (0, 0), (1, 0), (0, 0), (0, 0)))
    pair = jnp.concatenate([left, right], axis=-1).reshape(9, 4 * chans, 2 * chans)
    low = jnp.pad(pair, ((0, 0), (0, 2 * chans), (0, 0)))
    high = jnp.pad(pair, ((0, 0), (2 * chans, 0), (0, 0)))
    return jnp.concatenate([low, high], axis=-1).reshape(9 * WIN, OUT)


def conv_frame(ref, weight_ref, frame, taps=(0, 1, 2)):
    groups = (ref.shape[3] - 2 * OUT // 4) // OUT
    pieces = []
    for kt in taps:
        for kr in range(3):
            pieces.append(
                jnp.concatenate(
                    [ref[frame + kt, kr, :, OUT * j : OUT * j + WIN] for j in range(groups)],
                    axis=0,
                )
            )
    lhs = jnp.concatenate(pieces, axis=1)
    rhs = weight_ref[taps[0] * 3 * WIN : (taps[-1] + 1) * 3 * WIN, :]
    return jnp.dot(lhs, rhs, preferred_element_type=F32)


def first_kernel(
    chans,
    flag_ref,
    x_ref,
    back_ref,
    cache_ref,
    cot_ref,
    ahead_ref,
    w_first_ref,
    w_second_ref,
    bias_ref,
    pre_grad_ref,
    middle_ref,
    cache_grad_ref,
    act_ref,
    shifted_act,
    shifted_cot,
    slope_ref,
):
    frames, rows = x_ref.shape[0], x_ref.shape[1]
    groups = x_ref.shape[2] // OUT
    first = flag_ref[0] == 0

    def silu(value):
        value = value.astype(F32)
        return (value * logistic(value)).astype(BF16).astype(F32)

    @pl.when(first)
    def _():
        @pl.loop(0, 2)
        def _(f):
            put_shifted(shifted_act, f, silu(cache_ref[f]), chans)

    @pl.when(jnp.logical_not(first))
    def _():
        @pl.loop(0, 2)
        def _(f):
            put_shifted(shifted_act, f, silu(back_ref[f]), chans)

    @pl.loop(0, frames)
    def _(f):
        put_shifted(shifted_act, f + 2, silu(x_ref[f]), chans)
        put_shifted(shifted_cot, f, cot_ref[f].astype(F32), chans)

    @pl.loop(0, 2)
    def _(f):
        put_shifted(shifted_cot, f + frames, ahead_ref[f].astype(F32), chans)

    @pl.loop(0, frames + 2)
    def _(f):
        act_ref[f] = shifted_act[f, 1]

    @pl.loop(0, frames)
    def _(f):
        pre = conv_frame(shifted_act, w_first_ref, f) + bias_ref[...]
        s = logistic(pre)
        slope_ref[...] = s * (1.0 + pre * (1.0 - s))
        middle = (pre * s).astype(BF16)
        for j in range(groups):
            middle_ref[f, :, OUT * j : OUT * (j + 1)] = middle[rows * j : rows * (j + 1)]
        grad = conv_frame(shifted_cot, w_second_ref, f)
        pre_grad = (grad * slope_ref[...]).astype(BF16)
        for j in range(groups):
            pre_grad_ref[f, :, OUT * j : OUT * (j + 1)] = pre_grad[rows * j : rows * (j + 1)]

    for f in range(2):
        grad = conv_frame(shifted_cot, w_second_ref, f - 2, taps=(1, 2) if f else (2,))
        grad = grad.astype(BF16)
        for j in range(groups):
            cache_grad_ref[f, :, OUT * j : OUT * (j + 1)] = grad[rows * j : rows * (j + 1)]


def sums_kernel(
    chans,
    flag_ref,
    act_ref,
    pre_grad_ref,
    middle_ref,
    middle_cache_ref,
    cot_ref,
    ahead_ref,
    out_ref,
    mid,
    shifted_cot,
    shifted_grad,
    total_first,
    total_second,
):
    frames, rows = middle_ref.shape[0], middle_ref.shape[1]
    groups = middle_ref.shape[2] // OUT
    first = flag_ref[0] == 0

    @pl.loop(0, 2)
    def _(f):
        value = jnp.where(first, middle_cache_ref[f].astype(F32), 0.0)
        mid[f] = column_shift(value, chans).astype(BF16)

    @pl.loop(0, frames)
    def _(f):
        mid[f + 2] = column_shift(middle_ref[f].astype(F32), chans).astype(BF16)
        for k, part in enumerate(row_shifts(cot_ref[f].astype(F32))):
            shifted_cot[f, 2 - k] = part.astype(BF16)
        for k, part in enumerate(row_shifts(pre_grad_ref[f].astype(F32))):
            shifted_grad[f, 2 - k] = part.astype(BF16)

    @pl.loop(0, 2)
    def _(f):
        for k, part in enumerate(row_shifts(ahead_ref[f].astype(F32))):
            shifted_cot[f + frames, 2 - k] = part.astype(BF16)

    def correlate(source, upstream, pairs):
        left = jnp.concatenate(
            [source[a, :, OUT * j : OUT * j + WIN] for a, _ in pairs for j in range(groups)],
            axis=0,
        )
        right = jnp.concatenate(
            [
                jnp.concatenate(
                    [upstream[t, k, :, OUT * j : OUT * (j + 1)] for _, t in pairs for j in range(groups)],
                    axis=0,
                )
                for k in range(3)
            ],
            axis=1,
        )
        return lax.dot_general(
            left, right, (((0,), (0,)), ((), ())), preferred_element_type=F32
        )

    lane = lax.broadcasted_iota(jnp.int32, (chans, 2 * chans), 1) < chans

    def tap(total, kr, kq):
        cut = lambda d: total[
            chans * (kq + d) : chans * (kq + d + 1),
            OUT * kr + 2 * chans * (d // 2) : OUT * kr + 2 * chans * (d // 2 + 1),
        ]
        value = jnp.where(lane, cut(0) + cut(2), cut(1) + cut(3))
        return value + pltpu.roll(value, chans, axis=1)

    for kt in range(3):
        total_first[...] = correlate(act_ref, shifted_grad, [(t + kt, t) for t in range(frames)])
        total_second[...] = correlate(
            mid, shifted_cot, [(a, a - kt) for a in range(kt, frames + 2)]
        )
        for kr in range(3):
            for kq in range(3):
                at = ((kt * 3 + kr) * 3 + kq) * chans
                out_ref[at : at + chans, :] = jnp.where(
                    lane, tap(total_first, kr, kq), tap(total_second, kr, kq)
                ).astype(BF16)


def last_kernel(
    chans,
    x_ref,
    cache_ref,
    cot_ref,
    pre_grad_ref,
    ahead_ref,
    w_first_ref,
    input_grad_ref,
    cache_grad_ref,
    shifted,
):
    frames, rows = x_ref.shape[0], x_ref.shape[1]
    groups = x_ref.shape[2] // OUT

    @pl.loop(0, frames)
    def _(f):
        put_shifted(shifted, f, pre_grad_ref[f].astype(F32), chans)

    @pl.loop(0, 2)
    def _(f):
        put_shifted(shifted, f + frames, ahead_ref[f].astype(F32), chans)

    @pl.loop(0, frames)
    def _(f):
        grad = conv_frame(shifted, w_first_ref, f)
        for j in range(groups):
            cut = slice(OUT * j, OUT * (j + 1))
            value = grad[rows * j : rows * (j + 1)] * slope_of(x_ref[f, :, cut].astype(F32))
            input_grad_ref[f, :, cut] = (cot_ref[f, :, cut].astype(F32) + value).astype(BF16)

    for f in range(2):
        grad = conv_frame(shifted, w_first_ref, f - 2, taps=(1, 2) if f else (2,))
        for j in range(groups):
            cut = slice(OUT * j, OUT * (j + 1))
            value = grad[rows * j : rows * (j + 1)] * slope_of(cache_ref[f, :, cut].astype(F32))
            cache_grad_ref[f, :, cut] = value.astype(BF16)


def call(kernel, name, out_shape, scratch, n_smem, flops, args):
    moved = sum(a.size * a.dtype.itemsize for a in args)
    moved += sum(o.size * o.dtype.itemsize for o in jax.tree.leaves(out_shape))
    return pl.pallas_call(
        kernel,
        out_shape=out_shape,
        in_specs=[SMEM] * n_smem + [VMEM] * (len(args) - n_smem),
        out_specs=jax.tree.map(lambda _: VMEM, out_shape),
        scratch_shapes=scratch,
        compiler_params=PARAMS,
        cost_estimate=pl.CostEstimate(flops=flops, bytes_accessed=moved, transcendentals=0),
        name=name,
    )(*args)


def to_row_parts(grad, count):
    rows = grad.shape[1] // count
    mine = grad[:, :rows]
    place = lax.axis_index("tm")
    for k in range(1, count):
        part = lax.ppermute(grad[:, k * rows : (k + 1) * rows], "tm", [(0, k)])
        mine = jnp.where(place == k, part, mine)
    return mine[None]


def body(
    block_input, input_cache, middle_cache, first_weight, first_bias, second_weight, cotangent
):
    chans = first_weight.shape[3]
    tm, clips = lax.axis_size("tm"), lax.axis_size("clip")
    _, frames, rows, lanes = block_input.shape
    width = lanes // chans
    factor = 1.0 / math.sqrt(block_input.shape[0] * clips * frames * tm * rows * width)
    x, cot = block_input[0], cotangent[0]
    icache, mcache = input_cache[0], middle_cache[0]
    place = lax.axis_index("tm").astype(jnp.int32).reshape(1)
    onward = [(i, i + 1) for i in range(tm - 1)]
    backward = [(i + 1, i) for i in range(tm - 1)]
    back = lax.ppermute(x[frames - 2 :], "tm", onward)
    ahead = lax.ppermute(cot[:2], "tm", backward)

    def turned(weight):
        return jnp.transpose(jnp.flip(weight, (0, 1, 2)), (0, 1, 2, 4, 3))

    w_first, w_second = banded(first_weight), banded(turned(second_weight))
    w_first_turned = banded(turned(first_weight))
    bias = jnp.tile(first_bias, OUT // chans).reshape(1, OUT)

    padded = lanes + 2 * chans
    shape = lambda n, l=lanes: jax.ShapeDtypeStruct((n, rows, l), BF16)
    tap_flops = 2 * rows * width * 9 * chans * chans * 3
    pre_grad, middle, mid_cache_grad, act = call(
        functools.partial(first_kernel, chans),
        "first",
        (shape(frames), shape(frames), shape(2), shape(frames + 2, padded)),
        [
            pltpu.VMEM((frames + 2, 3, rows, padded), BF16),
            pltpu.VMEM((frames + 2, 3, rows, padded), BF16),
            pltpu.VMEM((rows * lanes // OUT, OUT), F32),
        ],
        1,
        tap_flops * 15,
        (place, x, back, icache, cot, ahead, w_first, w_second, bias),
    )
    grad_ahead = lax.ppermute(pre_grad[:2], "tm", backward)
    sums = call(
        functools.partial(sums_kernel, chans),
        "sums",
        jax.ShapeDtypeStruct((27 * chans, 2 * chans), BF16),
        [
            pltpu.VMEM((frames + 2, rows, padded), BF16),
            pltpu.VMEM((frames + 2, 3, rows, lanes), BF16),
            pltpu.VMEM((frames, 3, rows, lanes), BF16),
            pltpu.VMEM((WIN, 3 * OUT), F32),
            pltpu.VMEM((WIN, 3 * OUT), F32),
        ],
        1,
        tap_flops * 15,
        (place, act, pre_grad, middle, mcache, cot, ahead),
    )
    everyone = ("clip", "tm")
    count = clips * tm
    height = sums.shape[0]
    share = -(-height // count)
    padded_sums = jnp.pad(sums, ((0, share * count - height), (0, 0)))
    parts = lax.all_to_all(
        padded_sums.reshape(count, share, 2 * chans), everyone, 0, 0, tiled=True
    )
    mine = (jnp.sum(parts.astype(F32), axis=0) * factor).astype(BF16)
    whole = lax.all_to_all(
        jnp.broadcast_to(mine[None], (count, share, 2 * chans)), everyone, 0, 0, tiled=True
    )
    whole = whole.reshape(count * share, 2 * chans)[:height].reshape(3, 3, 3, chans, 2 * chans)
    first_total = whole[..., :chans].astype(F32)
    second_total = whole[..., chans:].astype(F32)

    input_grad, in_cache_grad = call(
        functools.partial(last_kernel, chans),
        "last",
        (shape(frames), shape(2)),
        [pltpu.VMEM((frames + 2, 3, rows, padded), BF16)],
        0,
        tap_flops * 9,
        (x, icache, cot, pre_grad, grad_ahead, w_first_turned),
    )
    return (
        input_grad[None],
        to_row_parts(in_cache_grad, tm),
        to_row_parts(mid_cache_grad, tm),
        first_total,
        second_total,
    )


def solution(mesh):
    return jax.shard_map(
        body,
        mesh=mesh,
        in_specs=(
            P("clip", "tm", None, None),
            P("clip", None, None, None),
            P("clip", None, None, None),
            P(),
            P(),
            P(),
            P("clip", "tm", None, None),
        ),
        out_specs=(
            P("clip", "tm", None, None),
            P("clip", None, "tm", None),
            P("clip", None, "tm", None),
            P(),
            P(),
        ),
        check_vma=False,
    )
```

```python
import functools
import math

import jax
import jax.numpy as jnp
from jax import lax
from jax.experimental import pallas as pl
from jax.experimental.pallas import tpu as pltpu
from jax.sharding import Mesh, PartitionSpec as P

F32 = jnp.float32
BF16 = jnp.bfloat16
OUT = 256
WIN = 384
VMEM = pl.BlockSpec(memory_space=pltpu.VMEM)
SMEM = pl.BlockSpec(memory_space=pltpu.SMEM)


def logistic(value):
    return 1.0 / (1.0 + jnp.exp(-value))


def slope_of(value):
    s = logistic(value)
    return s * (1.0 + value * (1.0 - s))


def row_shifts(value):
    rows = value.shape[0]
    row = lax.broadcasted_iota(jnp.int32, value.shape, 0)
    down = jnp.where(row == 0, 0.0, pltpu.roll(value, 1, axis=0))
    up = jnp.where(row == rows - 1, 0.0, pltpu.roll(value, rows - 1, axis=0))
    return down, value, up


def column_shift(value, chans):
    pad = jnp.zeros((value.shape[0], 2 * chans), value.dtype)
    return pltpu.roll(jnp.concatenate([value, pad], axis=1), chans, axis=1)


def put_shifted(ref, frame, value, chans):
    for k, part in enumerate(row_shifts(column_shift(value, chans))):
        ref[frame, k] = part.astype(BF16)


def spread(weight_ref, tap):
    chans = weight_ref.shape[1]
    zero = jnp.zeros((chans, chans), F32)
    left = [
        jnp.concatenate([weight_ref[3 * tap + kq].astype(F32), zero], axis=1) for kq in range(3)
    ]
    right = [pltpu.roll(value, chans, axis=1) for value in left]
    return left, right


def band_forward(weight_ref, out_ref):
    chans = weight_ref.shape[1]
    half = 2 * chans
    for tap in range(9):
        left, right = spread(weight_ref, tap)
        pairs = [left[0], left[1] + right[0], left[2] + right[1], right[2]]
        at = tap * WIN
        for c, pair in enumerate(pairs):
            pair = pair.astype(BF16)
            out_ref[at + chans * c : at + chans * (c + 1), :half] = pair
            out_ref[at + half + chans * c : at + half + chans * (c + 1), half:] = pair
        zero = jnp.zeros((half, half), BF16)
        out_ref[at + OUT : at + WIN, :half] = zero
        out_ref[at : at + half, half:] = zero


def band_turned(weight_ref, out_ref):
    chans = weight_ref.shape[1]
    half = 2 * chans
    zero = jnp.zeros((chans, half), BF16)
    for tap in range(9):
        left, right = spread(weight_ref, 8 - tap)
        even = ((left[2] + right[1]).astype(BF16), left[0].astype(BF16))
        odd = (right[2].astype(BF16), (left[1] + right[0]).astype(BF16))
        at = tap * WIN
        for d, tiles in enumerate((even + (zero,), odd + (zero,), (zero,) + even, (zero,) + odd)):
            for m, tile in enumerate(tiles):
                out_ref[chans * d : chans * (d + 1), at + half * m : at + half * (m + 1)] = tile


def conv(frame_of, weight_ref, taps, turned=False):
    pieces = []
    for kt in taps:
        ref, frame = frame_of(kt)
        groups = ref.shape[3] // OUT
        for kr in range(3):
            pieces.append(
                jnp.concatenate(
                    [ref[frame, kr, :, OUT * j : OUT * j + WIN] for j in range(groups)], axis=0
                )
            )
    lhs = jnp.concatenate(pieces, axis=1)
    span = slice(taps[0] * 3 * WIN, (taps[-1] + 1) * 3 * WIN)
    if turned:
        return lax.dot_general(
            lhs, weight_ref[:, span], (((1,), (1,)), ((), ())), preferred_element_type=F32
        )
    return jnp.dot(lhs, weight_ref[span, :], preferred_element_type=F32)


def silu(value):
    value = value.astype(F32)
    return (value * logistic(value)).astype(BF16).astype(F32)


def put_rows(ref, frame, value):
    for k, part in enumerate(row_shifts(value)):
        ref[frame, 2 - k] = part.astype(BF16)


def put_groups(ref, frame, value):
    rows = ref.shape[1]
    for j in range(ref.shape[2] // OUT):
        ref[frame, :, OUT * j : OUT * (j + 1)] = value[rows * j : rows * (j + 1)]


def own_kernel(
    place_ref,
    stack_ref,
    input_cache_ref,
    weight_ref,
    band_first_ref,
    band_second_ref,
    act_ref,
    cot_cols_ref,
    cot_rows_ref,
    pre_ref,
    grad_ref,
    cache_grad_ref,
    cache_sum_ref,
    cache_ref,
):
    frames, chans = cot_cols_ref.shape[0], weight_ref.shape[1]
    w_first_ref, w_second_ref = weight_ref.at[:27], weight_ref.at[27:]
    band_forward(w_first_ref, band_first_ref)
    band_turned(w_second_ref, band_second_ref)
    first = place_ref[0] == 0

    @pl.loop(0, frames)
    def _(f):
        put_shifted(act_ref, f + 2, silu(stack_ref[f]), chans)
        value = stack_ref[frames + f].astype(F32)
        put_shifted(cot_cols_ref, f, value, chans)
        put_rows(cot_rows_ref, f, value)

    @pl.loop(0, 2)
    def _(f):
        value = jnp.where(first, stack_ref[2 * frames + f].astype(F32), 0.0)
        cache_ref[f] = column_shift(value, chans).astype(BF16)

    for f in range(frames):
        taps = tuple(kt for kt in range(3) if f + kt >= 2)
        pre_ref[f] = conv(lambda kt: (act_ref, f + kt), band_first_ref, taps)
        taps = tuple(kt for kt in range(3) if f + kt < frames)
        grad_ref[f] = conv(lambda kt: (cot_cols_ref, f + kt), band_second_ref, taps, True)

    @pl.when(first)
    def _():
        @pl.loop(0, 2)
        def _(f):
            put_shifted(act_ref, f, silu(input_cache_ref[f]), chans)

        for f in range(min(2, frames)):
            taps = tuple(kt for kt in range(3) if f + kt < 2)
            pre_ref[f] += conv(lambda kt: (act_ref, f + kt), band_first_ref, taps)

    for f in range(2):
        taps = (1, 2) if f else (2,)
        grad = conv(lambda kt: (cot_cols_ref, f + kt - 2), band_second_ref, taps, True)
        put_groups(cache_grad_ref, f, grad.astype(BF16))
    for kt in range(2):
        cache_sum_ref[kt] = correlate(
            [(cache_ref, (a,)) for a in range(kt, 2)],
            [(cot_rows_ref, a - kt) for a in range(kt, 2)],
        )


def halo_kernel(
    place_ref,
    halo_ref,
    bias_ref,
    band_first_ref,
    band_second_ref,
    act_own_ref,
    pre_ref,
    grad_ref,
    pre_grad_ref,
    act_ref,
    middle_ref,
    cot_rows_ref,
    grad_rows_ref,
    shifted,
    pre_total,
    grad_total,
    flat,
):
    frames, chans = pre_ref.shape[0], OUT // 4
    first, end = place_ref[0] == 0, place_ref[0] == place_ref[1] - 1
    ahead = halo_ref.shape[0] - 2
    pre_total[...] = pre_ref[...]
    grad_total[...] = grad_ref[...]

    @pl.when(first)
    def _():
        for f in range(2):
            act_ref[f] = act_own_ref[f, 1]

    @pl.when(jnp.logical_not(first))
    def _():
        @pl.loop(0, 2)
        def _(f):
            put_shifted(shifted, f, silu(halo_ref[f]), chans)
            act_ref[f] = shifted[f, 1]

        for f in range(min(2, frames)):
            taps = tuple(kt for kt in range(3) if f + kt < 2)
            pre_total[f] += conv(lambda kt: (shifted, f + kt), band_first_ref, taps)

    @pl.when(end)
    def _():
        cot_rows_ref[...] = jnp.zeros(cot_rows_ref.shape, BF16)

    @pl.when(jnp.logical_not(end))
    def _():
        @pl.loop(0, 2)
        def _(f):
            value = halo_ref[ahead + f].astype(F32)
            put_shifted(shifted, f, value, chans)
            put_rows(cot_rows_ref, f, value)

        for f in range(max(0, frames - 2), frames):
            taps = tuple(kt for kt in range(3) if f + kt >= frames)
            grad_total[f] += conv(
                lambda kt: (shifted, f + kt - frames), band_second_ref, taps, True
            )

    bias = jnp.concatenate([bias_ref[...], jnp.zeros((1, chans), F32)], axis=1)
    bias = bias + pltpu.roll(bias, chans, axis=1)
    bias = jnp.concatenate([bias] * (OUT // (2 * chans)), axis=1)

    @pl.loop(0, frames)
    def _(f):
        pre, grad = pre_total[f] + bias, grad_total[f]
        s = logistic(pre)
        put_groups(pre_grad_ref, f, (grad * (s * (1.0 + pre * (1.0 - s)))).astype(BF16))
        put_groups(flat, 0, pre * s)
        middle_ref[f] = column_shift(flat[0], chans).astype(BF16)
        put_rows(grad_rows_ref, f, pre_grad_ref[f].astype(F32))


def correlate(sources, upstreams):
    groups = upstreams[0][0].shape[3] // OUT
    left = jnp.concatenate(
        [
            ref[at + (slice(None), slice(OUT * j, OUT * j + WIN))]
            for ref, at in sources
            for j in range(groups)
        ],
        axis=0,
    )
    right = jnp.concatenate(
        [
            jnp.concatenate(
                [
                    ref[t, k, :, OUT * j : OUT * (j + 1)]
                    for ref, t in upstreams
                    for j in range(groups)
                ],
                axis=0,
            )
            for k in range(3)
        ],
        axis=1,
    )
    return lax.dot_general(
        left, right, (((0,), (0,)), ((), ())), preferred_element_type=F32
    )


def sums_kernel(
    act_ref,
    act_back_ref,
    middle_ref,
    cot_ref,
    cot_ahead_ref,
    grad_ref,
    cache_sum_ref,
    out_ref,
    total_first,
    total_second,
):
    frames = middle_ref.shape[0]
    chans = OUT // 4
    lane = lax.broadcasted_iota(jnp.int32, (chans, 2 * chans), 1) < chans

    def tap(total, kr, kq):
        cut = lambda d: total[
            chans * (kq + d) : chans * (kq + d + 1),
            OUT * kr + 2 * chans * (d // 2) : OUT * kr + 2 * chans * (d // 2 + 1),
        ]
        value = jnp.where(lane, cut(0) + cut(2), cut(1) + cut(3))
        return value + pltpu.roll(value, chans, axis=1)

    acts = [(act_back_ref, (f,)) for f in range(2)]
    acts += [(act_ref, (f + 2, 1)) for f in range(frames)]
    mids = [(middle_ref, (f,)) for f in range(frames)]
    cots = [(cot_ref, f) for f in range(frames)] + [(cot_ahead_ref, f) for f in range(2)]
    grads = [(grad_ref, f) for f in range(frames)]
    used, whole = 27 * chans, out_ref.shape[0]
    for kt in range(3):
        total_first[...] = correlate(acts[kt : kt + frames], grads)
        second = correlate(mids, cots[2 - kt : 2 - kt + frames])
        total_second[...] = second + cache_sum_ref[kt] if kt < 2 else second
        for kr in range(3):
            for kq in range(3):
                at = ((kt * 3 + kr) * 3 + kq) * chans
                out_ref[at : at + chans, :] = jnp.where(
                    lane, tap(total_first, kr, kq), tap(total_second, kr, kq)
                ).astype(BF16)
    if whole > used:
        out_ref[used:, :] = jnp.zeros((whole - used, 2 * chans), BF16)


def share_kernel(factor, parts_ref, out_ref):
    total = parts_ref[0].astype(F32)
    for k in range(1, parts_ref.shape[0]):
        total = total + parts_ref[k].astype(F32)
    total = (total * factor).astype(BF16)
    for k in range(out_ref.shape[0]):
        out_ref[k] = total


def last_kernel(
    stack_ref,
    cache_ref,
    pre_grad_ref,
    ahead_ref,
    weight_ref,
    input_grad_ref,
    cache_grad_ref,
    shifted,
    band,
):
    frames, rows, lanes = pre_grad_ref.shape
    chans = weight_ref.shape[1]
    groups = lanes // OUT
    band_turned(weight_ref, band)

    @pl.loop(0, frames)
    def _(f):
        put_shifted(shifted, f, pre_grad_ref[f].astype(F32), chans)

    @pl.loop(0, 2)
    def _(f):
        put_shifted(shifted, f + frames, ahead_ref[f].astype(F32), chans)

    @pl.loop(0, frames)
    def _(f):
        grad = conv(lambda kt: (shifted, f + kt), band, (0, 1, 2), True)
        for j in range(groups):
            cut = slice(OUT * j, OUT * (j + 1))
            value = grad[rows * j : rows * (j + 1)] * slope_of(stack_ref[f, :, cut].astype(F32))
            cot = stack_ref[frames + f, :, cut].astype(F32)
            input_grad_ref[f, :, cut] = (cot + value).astype(BF16)

    for f in range(2):
        grad = conv(lambda kt: (shifted, f + kt - 2), band, (1, 2) if f else (2,), True)
        for j in range(groups):
            cut = slice(OUT * j, OUT * (j + 1))
            value = grad[rows * j : rows * (j + 1)] * slope_of(cache_ref[f, :, cut].astype(F32))
            cache_grad_ref[f, :, cut] = value.astype(BF16)


def call(kernel, name, out_shape, scratch, flops, args, limit=20):
    smem = [a.dtype == jnp.int32 for a in args]
    moved = sum(a.size * a.dtype.itemsize for a in args)
    moved += sum(o.size * o.dtype.itemsize for o in jax.tree.leaves(out_shape))
    return pl.pallas_call(
        kernel,
        out_shape=out_shape,
        in_specs=[SMEM if s else VMEM for s in smem],
        out_specs=jax.tree.map(lambda _: VMEM, out_shape),
        scratch_shapes=scratch,
        compiler_params=pltpu.CompilerParams(vmem_limit_bytes=limit * 1024 * 1024),
        cost_estimate=pl.CostEstimate(flops=flops, bytes_accessed=moved, transcendentals=0),
        name=name,
    )(*args)


def to_row_parts(grads, count):
    rows = grads.shape[1] // count
    mine = grads[:, :rows]
    place = lax.axis_index("tm")
    for k in range(1, count):
        part = lax.ppermute(grads[:, k * rows : (k + 1) * rows], "tm", [(0, k)])
        mine = jnp.where(place == k, part, mine)
    return mine


def body(
    block_input, input_cache, middle_cache, first_weight, first_bias, second_weight, cotangent
):
    chans = first_weight.shape[3]
    tm, chips, cores = (lax.axis_size(axis) for axis in ("tm", "chip", "core"))
    clips = chips * cores
    _, frames, rows, lanes = block_input.shape
    width = lanes // chans
    factor = 1.0 / math.sqrt(block_input.shape[0] * clips * frames * tm * rows * width)
    x, cot = block_input[0], cotangent[0]
    icache, mcache = input_cache[0], middle_cache[0]
    w_first = first_weight.reshape(27, chans, chans)
    w_second = second_weight.reshape(27, chans, chans)
    index = lax.axis_index("tm").astype(jnp.int32)
    core = lax.axis_index("core").astype(jnp.int32)
    place = jnp.stack([index, jnp.int32(tm)])
    onward = [(i, i + 1) for i in range(tm - 1)]
    backward = [(i + 1, i) for i in range(tm - 1)]
    if tm == 2:
        sent = jnp.where(index == 0, x[frames - 2 :], cot[:2])
        halo = lax.ppermute(sent, "tm", onward + backward)
    else:
        back = lax.ppermute(x[frames - 2 :], "tm", onward)
        halo = jnp.concatenate([back, lax.ppermute(cot[:2], "tm", backward)])

    stack, weights = jnp.concatenate([x, cot, mcache]), jnp.concatenate([w_first, w_second])
    padded = lanes + 2 * chans
    make = lambda *s, t=BF16: jax.ShapeDtypeStruct(s, t)
    tap_flops = 2 * rows * width * 9 * chans * chans * 3
    positions = rows * lanes // OUT
    (
        band_first,
        band_second,
        act,
        cot_cols,
        cot_rows,
        pre,
        grad,
        mid_cache_grad,
        cache_sum,
    ) = call(
        own_kernel,
        "own",
        (
            make(9 * WIN, OUT),
            make(OUT, 9 * WIN),
            make(frames + 2, 3, rows, padded),
            make(frames, 3, rows, padded),
            make(frames, 3, rows, lanes),
            make(frames, positions, OUT, t=F32),
            make(frames, positions, OUT, t=F32),
            make(2, rows, lanes),
            make(2, WIN, 3 * OUT, t=F32),
        ),
        [
            pltpu.VMEM((2, rows, padded), BF16),
        ],
        tap_flops * 12,
        (
            place,
            stack,
            icache,
            weights,
        ),
    )
    pre_grad, act_back, middle, cot_ahead, grad_rows = call(
        halo_kernel,
        "halo",
        (
            make(frames, rows, lanes),
            make(2, rows, padded),
            make(frames, rows, padded),
            make(2, 3, rows, lanes),
            make(frames, 3, rows, lanes),
        ),
        [
            pltpu.VMEM((2, 3, rows, padded), BF16),
            pltpu.VMEM((frames, positions, OUT), F32),
            pltpu.VMEM((frames, positions, OUT), F32),
            pltpu.VMEM((1, rows, lanes), F32),
        ],
        tap_flops * 6,
        (
            place,
            halo,
            first_bias.reshape(1, chans),
            band_first,
            band_second,
            act,
            pre,
            grad,
        ),
    )
    grad_ahead = lax.ppermute(pre_grad[:2], "tm", backward)
    count = clips * tm
    share = -(-27 * chans // (8 * count)) * 8
    sums = call(
        sums_kernel,
        "sums",
        make(count * share, 2 * chans),
        [pltpu.VMEM((WIN, 3 * OUT), F32), pltpu.VMEM((WIN, 3 * OUT), F32)],
        tap_flops * 12,
        (act, act_back, middle, cot_rows, cot_ahead, grad_rows, cache_sum),
    )
    parts = lax.all_to_all(
        sums.reshape(count, share, 2 * chans), ("core", "chip", "tm"), 0, 0, tiled=True
    )
    shares = call(
        functools.partial(share_kernel, factor),
        "share",
        make(count // cores, share, 2 * chans),
        [],
        count * share * 2 * chans,
        (parts,),
        limit=60,
    )
    whole = lax.all_to_all(shares, ("chip", "tm"), 0, 0, tiled=True)
    whole = whole.reshape(count // cores * share, 2 * chans)
    if cores == 2:
        other = lax.ppermute(whole, "core", [(0, 1), (1, 0)])
        low, high = jnp.where(core == 0, whole, other), jnp.where(core == 0, other, whole)
        whole = jnp.concatenate([low, high])
    whole = whole[: 27 * chans].reshape(3, 3, 3, chans, 2 * chans)
    first_total = whole[..., :chans].astype(F32)
    second_total = whole[..., chans:].astype(F32)

    input_grad, in_cache_grad = call(
        last_kernel,
        "last",
        (make(frames, rows, lanes), make(2, rows, lanes)),
        [pltpu.VMEM((frames + 2, 3, rows, padded), BF16), pltpu.VMEM((OUT, 9 * WIN), BF16)],
        tap_flops * 9,
        (stack, icache, pre_grad, grad_ahead, weights),
    )
    cache_grads = to_row_parts(jnp.concatenate([in_cache_grad, mid_cache_grad]), tm)
    return (
        input_grad[None],
        cache_grads[None, :2],
        cache_grads[None, 2:],
        first_total,
        second_total,
    )


def solution(mesh):
    clips, tm = mesh.devices.shape
    cores = 2 if clips % 2 == 0 else 1
    split = Mesh(mesh.devices.reshape(clips // cores, cores, tm), ("chip", "core", "tm"))
    clip = ("chip", "core")
    return jax.shard_map(
        body,
        mesh=split,
        in_specs=(
            P(clip, "tm", None, None),
            P(clip, None, None, None),
            P(clip, None, None, None),
            P(),
            P(),
            P(),
            P(clip, "tm", None, None),
        ),
        out_specs=(
            P(clip, "tm", None, None),
            P(clip, None, "tm", None),
            P(clip, None, "tm", None),
            P(),
            P(),
        ),
        check_vma=False,
    )
```
